32 devices in a mesh: row: 4 (over y, core), col: 8 (over z, x).
Axes of the slice: x: 2, y: 2, z: 4, core: 2. Of those that a mesh axis runs over, the one named last changes fastest.
Arguments:
- residuals: bfloat16 [16384, 32], P(('row', 'col')), may hold values from -6 to 6
- intersect_blocks: int32 [32, 4], P(('row', 'col')), may hold values from 0 to 3
- local_inverse: bfloat16 [16384, 1024], P(('row', 'col')), may hold values from -0.1875 to 0.1875
- coarse_basis: float32 [32768, 64], P(('row', 'col')), may hold values from -0.1875 to 0.1875
- coarse_slots: int32 [2048], replicated, may hold values from 0 to 2047, each once
- coarse_inverse: float32 [2048, 2048], P('row', 'col'), may hold values from -0.5 to 0.5
Outputs:
- preconditioned: float32 [16384, 32], P(('row', 'col'))
The draws below stay inside these ranges and needn't reach their ends.
Inputs may be any that keep to these rules, and one draw needn't show every extreme that they name: `intersect_blocks`: each entry names one of the four owned blocks. `coarse_slots`: every coarse index from 0 to 2047 appears exactly once.
All inputs are finite; a program needn't handle non-finite values.
Results may differ from the reference program's by a relative error of at most 0.0003.
Values may be sent and summed in bfloat16 or wider, within the bound.
A program may use at most 64 MiB of HBM per device.

```python
import jax
import jax.numpy as jnp
from jax import lax

BLK = 128
OWN = 512
LOC = 1024
RHS = 32
NEV = 64
COARSE = 2048
DOFS = 16384
N_ROW = 4
N_COL = 8
DEVICES = 32


def set_ends(array, rng, smallest, largest):
    shape = array.shape
    spot = [jax.random.randint(jax.random.fold_in(rng, axis), (), 0, shape[axis]) for axis in range(len(shape))]
    array = array.at[tuple(spot)].set(smallest)
    longest = shape.index(max(shape))
    spot[longest] = (spot[longest] + 1) % shape[longest]
    return array.at[tuple(spot)].set(largest)


def shard_levels(own_key, extent, shards, smallest, high):
    loudness = 1.0
    for position, parts in shards:
        steps = jax.random.uniform(jax.random.fold_in(jax.random.fold_in(own_key, 6), position), (parts,), jnp.float32, smallest / len(shards), high / len(shards))
        loudness = loudness * jnp.repeat(jnp.exp(steps), extent[position] // parts).reshape((-1,) + (1,) * (len(extent) - 1 - position))
    return loudness


def bell_draw(own_key, shape, scale, bound, split=(), kind=jnp.bfloat16):
    array = jax.random.normal(own_key, shape, jnp.float32) * scale
    if len(split) > 0:
        array = shard_levels(own_key, shape, split, -0.22, 0.18) * array
    return jnp.clip(array, min=-bound, max=bound).astype(kind)


def setup_inputs(seed: int = 0) -> dict:
    keys = jax.random.split(jax.random.key(seed), 7)
    return {
        "residuals": bell_draw(keys[0], (DOFS, RHS), 1.0, 6.0, ((0, 32),)),
        "intersect_blocks": set_ends(jax.random.randint(keys[1], (DEVICES, 4), 0, 4), jax.random.fold_in(keys[1], 1), 0, 3).astype(jnp.int32),
        "local_inverse": bell_draw(keys[2], (DOFS, LOC), LOC ** -0.5, 0.1875, ((0, 32),)),
        "coarse_basis": bell_draw(keys[3], (DEVICES * LOC, NEV), LOC ** -0.5, 0.1875, ((0, 32),), jnp.float32),
        "coarse_slots": jax.random.permutation(keys[4], COARSE).astype(jnp.int32),
        "coarse_inverse": bell_draw(keys[5], (COARSE, COARSE), (COARSE // 16) ** -0.5, 0.5, ((0, 4), (1, 8)), jnp.float32),
    }


def shift_grid(field, axis, by):
    count = field.shape[axis]
    moved = jnp.roll(field, by, axis=axis)
    source = jnp.arange(count, dtype=jnp.int32) - by
    valid = ((source >= 0) & (source < count)).astype(field.dtype)
    shape = [1] * field.ndim
    shape[axis] = count
    return moved * valid.reshape(shape)


def local_product(pair):
    return jnp.dot(pair[0], pair[1], preferred_element_type=jnp.float32)


def reference(residuals, intersect_blocks, local_inverse, coarse_basis, coarse_slots, coarse_inverse):
    nrows = N_ROW
    ncols = N_COL
    blocks = residuals.reshape(nrows, ncols, OWN // BLK, BLK, RHS)
    sends = intersect_blocks.reshape(nrows, ncols, 4).astype(jnp.int32)
    outgoing = jnp.take_along_axis(blocks, sends[:, :, :, None, None], axis=2)
    incoming = jnp.stack([shift_grid(outgoing[:, :, 0], 0, 1), shift_grid(outgoing[:, :, 1], 0, -1),
                          shift_grid(outgoing[:, :, 2], 1, 1), shift_grid(outgoing[:, :, 3], 1, -1)], axis=2)
    local_vec = jnp.concatenate([residuals.reshape(nrows, ncols, OWN, RHS),
                                 incoming.reshape(nrows, ncols, LOC - OWN, RHS)], axis=2).reshape(DEVICES, LOC, RHS)
    inverse = local_inverse.reshape(DEVICES, OWN, LOC)
    schwarz = lax.map(local_product, (inverse, local_vec))
    basis = coarse_basis.reshape(DEVICES, LOC, NEV)
    partial_value = jnp.einsum("dln,dlr->dnr", basis, local_vec.astype(jnp.float32), precision=lax.Precision.HIGHEST)
    coarse_rhs = jnp.zeros((COARSE, RHS), jnp.float32).at[coarse_slots].set(partial_value.reshape(COARSE, RHS))
    coarse_sol = jnp.dot(coarse_inverse, coarse_rhs, precision=lax.Precision.HIGHEST)
    own_coarse = coarse_sol[coarse_slots].reshape(DEVICES, NEV, RHS)
    prolonged = jnp.einsum("dln,dnr->dlr", basis, own_coarse, precision=lax.Precision.HIGHEST)
    grid = prolonged.reshape(nrows, ncols, LOC, RHS)
    returning = grid[:, :, OWN:].reshape(nrows, ncols, 4, BLK, RHS)
    returned = jnp.stack([shift_grid(returning[:, :, 0], 0, -1), shift_grid(returning[:, :, 1], 0, 1),
                          shift_grid(returning[:, :, 2], 1, -1), shift_grid(returning[:, :, 3], 1, 1)], axis=2)
    matches = (sends[..., None] == jnp.arange(OWN // BLK, dtype=jnp.int32)).astype(jnp.float32)
    added = jnp.einsum("rcdb,rcdkq->rcbkq", matches, returned, precision=lax.Precision.HIGHEST)
    result = schwarz.reshape(nrows, ncols, OWN, RHS) + grid[:, :, :OWN] + added.reshape(nrows, ncols, OWN, RHS)
    return result.reshape(DOFS, RHS)
```

```python
import functools

import jax
import jax.numpy as jnp
from jax import lax
from jax.experimental import pallas as pl
from jax.experimental.pallas import tpu as pltpu
from jax.sharding import PartitionSpec as P

MESH = pl.DeviceIdType.MESH
BLK = 128
LANES = 128
UNROLL = 16
NT = (((1,), (1,)), ((), ()))
NN = (((1,), (0,)), ((), ()))
F32 = jnp.float32
BF16 = jnp.bfloat16


def matmul(a, b, dims):
    return lax.dot_general(a, b, dims, preferred_element_type=F32)


def split(x):
    hi = x.astype(BF16)
    return hi, (x - hi.astype(F32)).astype(BF16)


def loop(start, stop, body):
    if stop - start <= UNROLL:
        for i in range(start, stop):
            body(i)
    else:
        def step(i, carry):
            body(i)
            return carry

        lax.fori_loop(start, stop, step, 0)


def flipped(index, k, count):
    out = index
    bit = 1
    while bit < count:
        kbit = (k // bit) % 2
        out = out + kbit * bit * (1 - 2 * ((index // bit) % 2))
        bit *= 2
    return out


def lane_low(shape):
    return lax.broadcasted_iota(jnp.int32, shape, len(shape) - 1) < LANES // 2


def half_roll(x):
    return pltpu.roll(x, LANES // 2, 1)


def kernel(
    nrow,
    ncol,
    res_ref,
    ib_ref,
    linv_hbm,
    basis_hbm,
    slots_ref,
    coarse_hbm,
    out_ref,
    outgoing,
    incoming,
    linv,
    basis,
    basis2,
    coarse,
    coarse_hi,
    coarse_lo,
    hot_in,
    hot_out,
    gathered,
    gathered2,
    pieces,
    received,
    solved,
    returning,
    returned,
    load_sem,
    halo_send,
    halo_recv,
    back_send,
    back_recv,
    ag1_send,
    ag1_recv,
    rs_send,
    rs_recv,
    ag2_send,
    ag2_recv,
):
    r = lax.axis_index("row")
    c = lax.axis_index("col")
    me = r * ncol + c
    rhs = res_ref.shape[0]
    own = res_ref.shape[1]
    half = rhs // 2
    ndev = nrow * ncol
    rows, width = coarse.shape
    total = slots_ref.shape[1]

    def col_peer(k):
        return (r, flipped(c, k, ncol))

    def row_peer(j):
        return (lax.rem(r + j, nrow), c)

    barrier = pltpu.get_barrier_semaphore()
    loop(1, ncol, lambda k: pl.semaphore_signal(barrier, inc=1, device_id=col_peer(ncol - k), device_id_type=MESH))
    loop(1, nrow, lambda j: pl.semaphore_signal(barrier, inc=1, device_id=row_peer(j), device_id_type=MESH))

    loads = [
        pltpu.make_async_copy(basis_hbm, basis, load_sem.at[0]),
        pltpu.make_async_copy(coarse_hbm, coarse, load_sem.at[1]),
        pltpu.make_async_copy(linv_hbm, linv, load_sem.at[2]),
    ]
    for load in loads:
        load.start()

    exists = [r < nrow - 1, r > 0, c < ncol - 1, c > 0]
    target = [(r + 1, c), (r - 1, c), (r, c + 1), (r, c - 1)]
    opposite = [1, 0, 3, 2]
    blocks = [res_ref[:, b * BLK:(b + 1) * BLK] for b in range(own // BLK)]
    for d in range(4):
        index = ib_ref[0, d]
        value = blocks[0]
        for b in range(1, len(blocks)):
            value = jnp.where(index == b, blocks[b], value)
        outgoing[d] = value

        @pl.when(jnp.logical_not(exists[opposite[d]]))
        def _():
            incoming[d] = jnp.zeros_like(incoming[d])

        @pl.when(jnp.logical_not(exists[d]))
        def _():
            returned[d] = jnp.zeros_like(returned[d])

    def halo(d):
        return pltpu.make_async_remote_copy(
            src_ref=outgoing.at[d], dst_ref=incoming.at[d],
            send_sem=halo_send.at[d], recv_sem=halo_recv.at[d],
            device_id=target[d], device_id_type=MESH)

    def back(d):
        return pltpu.make_async_remote_copy(
            src_ref=returning.at[d], dst_ref=returned.at[d],
            send_sem=back_send.at[d], recv_sem=back_recv.at[d],
            device_id=target[opposite[d]], device_id_type=MESH)

    pl.semaphore_wait(barrier, ncol + nrow - 2)
    for d in range(4):
        @pl.when(exists[d])
        def _():
            halo(d).start()

    loads[0].wait()
    nev = basis.shape[0]
    b_hi, b_lo = split(basis[...])
    basis2[:nev] = b_hi
    basis2[nev:] = b_lo
    partial = matmul(res_ref[...], basis2[:, :own], NT)

    for d in range(4):
        @pl.when(exists[opposite[d]])
        def _():
            halo(d).wait_recv()

    inc = jnp.concatenate([incoming[d] for d in range(4)], axis=1)
    partial = partial + matmul(inc, basis2[:, own:], NT)
    partial = partial + half_roll(partial)
    low = lane_low((half, LANES))
    gathered[me] = jnp.where(low, partial[:half], partial[half:])

    def spread(buf, send, recv):
        def to_col(k):
            return pltpu.make_async_remote_copy(
                src_ref=buf.at[me], dst_ref=buf.at[me],
                send_sem=send.at[k, 0], recv_sem=recv.at[me],
                device_id=col_peer(k), device_id_type=MESH)

        def to_row(k, j):
            slot = r * ncol + flipped(c, k, ncol)
            return pltpu.make_async_remote_copy(
                src_ref=buf.at[slot], dst_ref=buf.at[slot],
                send_sem=send.at[k, j], recv_sem=recv.at[slot],
                device_id=row_peer(j), device_id_type=MESH)

        def arrival(slot):
            pltpu.make_async_remote_copy(
                src_ref=buf.at[slot], dst_ref=buf.at[slot],
                send_sem=send.at[0, 0], recv_sem=recv.at[slot],
                device_id=row_peer(1), device_id_type=MESH).wait_recv()

        def start():
            loop(1, ncol, lambda i: to_col(ncol - i).start())
            for j in range(1, nrow):
                to_row(0, j).start()

        def relay(first, last):
            def one(k):
                arrival(r * ncol + flipped(c, k, ncol))
                for j in range(1, nrow):
                    to_row(k, j).start()

            loop(first, last, one)

        def finish():
            def one(k):
                for j in range(1, nrow):
                    arrival(lax.rem(r + j, nrow) * ncol + flipped(c, k, ncol))

            loop(0, ncol, one)

        def drain():
            def one(k):
                for j in range(1, nrow):
                    to_row(k, j).wait_send()

            loop(0, ncol, one)
            loop(1, ncol, lambda k: to_col(k).wait_send())

        return start, relay, finish, drain

    def unpacked(buf):
        def one(p):
            a, b = buf[2 * p], buf[2 * p + 1]
            top = jnp.where(low, a, half_roll(b))
            bot = jnp.where(low, half_roll(a), b)
            t_hi, t_lo = split(top)
            b_hi, b_lo = split(bot)
            lanes = pl.ds(p * LANES if isinstance(p, int) else pl.multiple_of(p * LANES, LANES), LANES)
            gathered2[0 * half:1 * half, lanes] = t_hi
            gathered2[1 * half:2 * half, lanes] = b_hi
            gathered2[2 * half:3 * half, lanes] = t_lo
            gathered2[3 * half:4 * half, lanes] = b_lo

        loop(0, ndev // 2, one)

    start1, relay1, finish1, drain1 = spread(gathered, ag1_send, ag1_recv)
    start1()

    loads[2].wait()
    local = jnp.concatenate([res_ref[...], inc], axis=1)
    out_ref[...] = matmul(local, linv[...], NT)
    relay1(1, ncol // 2)
    chunk = 2 * LANES

    def build_in(i):
        lanes = pl.ds(i * chunk if isinstance(i, int) else pl.multiple_of(i * chunk, chunk), chunk)
        slot = slots_ref[:, lanes] - c * width
        place = lax.broadcasted_iota(jnp.int32, (width, chunk), 0)
        hot_in[:, lanes] = jnp.where(place == slot, 1.0, 0.0).astype(BF16)

    loop(0, total // chunk, build_in)
    relay1(ncol // 2, ncol)
    loads[1].wait()
    a_hi, a_lo = split(coarse[...])
    coarse_hi[...] = a_hi
    coarse_lo[...] = a_lo
    finish1()

    unpacked(gathered)
    depth = min(total, 2048)
    column = matmul(gathered2[:, :depth], hot_in[:, :depth], NT)
    if total > depth:
        def more(i, acc):
            lanes = pl.ds(pl.multiple_of(i * depth, depth), depth)
            return acc + matmul(gathered2[:, lanes], hot_in[:, lanes], NT)

        column = lax.fori_loop(1, total // depth, more, column)
    column_hi, column_lo = split(column[:rhs] + column[rhs:])
    column2 = jnp.concatenate([column_hi, column_lo], axis=0)
    span = 2 * LANES

    def product(i):
        at = pl.ds(i * span if isinstance(i, int) else pl.multiple_of(i * span, span), span)
        part = matmul(column2, coarse_hi[at], NT) + matmul(column2, coarse_lo[at], NT)
        part = part[:rhs] + part[rhs:]
        for q in range(span // LANES):
            top = part[:half, q * LANES:(q + 1) * LANES]
            bot = part[half:, q * LANES:(q + 1) * LANES]
            pieces[(span // LANES * i + q) * 2] = jnp.where(low, top, half_roll(bot))
            pieces[(span // LANES * i + q) * 2 + 1] = jnp.where(low, half_roll(top), bot)

    loop(0, rows // span, product)

    def reduce(k):
        peer = flipped(c, k, ncol)
        return pltpu.make_async_remote_copy(
            src_ref=pieces.at[peer], dst_ref=received.at[c],
            send_sem=rs_send.at[k], recv_sem=rs_recv.at[c],
            device_id=(r, peer), device_id_type=MESH)

    def reduce_arrival(k):
        peer = flipped(c, k, ncol)
        pltpu.make_async_remote_copy(
            src_ref=pieces.at[peer], dst_ref=received.at[peer],
            send_sem=rs_send.at[k], recv_sem=rs_recv.at[peer],
            device_id=(r, peer), device_id_type=MESH).wait_recv()

    loop(1, ncol, lambda i: reduce(ncol - i).start())

    at = pl.ds(pl.multiple_of((me // 2) * LANES, LANES), LANES)
    mine = jnp.broadcast_to(slots_ref[:, at], (8, LANES))
    swapped = half_roll(mine)
    low8 = lane_low((8, LANES))
    mine = jnp.where(lax.rem(me, 2) == 0, jnp.where(low8, mine, swapped), jnp.where(low8, swapped, mine))[:1]
    tall = 4 * LANES

    def build_out(i):
        at = pl.ds(i * tall if isinstance(i, int) else pl.multiple_of(i * tall, tall), tall)
        place = lax.broadcasted_iota(jnp.int32, (tall, LANES), 0) + i * tall
        hot_out[at] = jnp.where(place == mine, 1.0, 0.0).astype(BF16)

    loop(0, total // tall, build_out)

    loop(1, ncol, reduce_arrival)
    summed = pieces[c]
    if ncol - 1 <= UNROLL:
        for k in range(1, ncol):
            summed = summed + received[flipped(c, k, ncol)]
    else:
        summed = lax.fori_loop(1, ncol, lambda k, acc: acc + received[flipped(c, k, ncol)], summed)
    solved[me] = summed

    start2, relay2, finish2, drain2 = spread(solved, ag2_send, ag2_recv)
    start2()
    relay2(1, ncol)
    finish2()
    unpacked(solved)
    picked = matmul(gathered2[:, :depth], hot_out[:depth], NN)
    if total > depth:
        def again(i, acc):
            at = pl.ds(pl.multiple_of(i * depth, depth), depth)
            return acc + matmul(gathered2[:, at], hot_out[at], NN)

        picked = lax.fori_loop(1, total // depth, again, picked)
    picked = picked.astype(BF16)

    outer = matmul(picked, basis2[:, own:], NN)
    outer = outer[:rhs] + outer[rhs:]
    for d in range(4):
        returning[d] = outer[:, d * BLK:(d + 1) * BLK]

        @pl.when(exists[opposite[d]])
        def _():
            back(d).start()

    inner = matmul(picked, basis2[:, :own], NN)
    out_ref[...] = out_ref[...] + inner[:rhs] + inner[rhs:]
    for d in range(4):
        @pl.when(exists[d])
        def _():
            back(d).wait_recv()

    for b in range(own // BLK):
        value = out_ref[:, b * BLK:(b + 1) * BLK]
        for d in range(4):
            value = value + jnp.where(ib_ref[0, d] == b, returned[d], 0.0)
        out_ref[:, b * BLK:(b + 1) * BLK] = value

    drain1()
    drain2()
    loop(1, ncol, lambda k: reduce(k).wait_send())
    for d in range(4):
        @pl.when(exists[d])
        def _():
            halo(d).wait_send()

        @pl.when(exists[opposite[d]])
        def _():
            back(d).wait_send()


def shards(nrow, ncol, residuals, intersect_blocks, local_inverse, coarse_basis, coarse_slots, coarse_inverse):
    own, rhs = residuals.shape
    loc, nev = coarse_basis.shape
    rows, width = coarse_inverse.shape
    total = coarse_slots.shape[0]
    ndev = nrow * ncol
    assert 2 * nev == LANES and rows == ncol * nev and loc == own + 4 * BLK and own % BLK == 0
    packed = (rhs // 2, LANES)
    vmem = pl.BlockSpec(memory_space=pltpu.VMEM)
    hbm = pl.BlockSpec(memory_space=pl.ANY)
    dma = pltpu.SemaphoreType.DMA
    out = pl.pallas_call(
        functools.partial(kernel, nrow, ncol),
        name="schwarz",
        out_shape=jax.ShapeDtypeStruct((rhs, own), F32),
        in_specs=[vmem, pl.BlockSpec(memory_space=pltpu.SMEM), hbm, hbm, vmem, hbm],
        out_specs=vmem,
        scratch_shapes=[
            pltpu.VMEM((4, rhs, BLK), BF16),
            pltpu.VMEM((4, rhs, BLK), BF16),
            pltpu.VMEM((own, loc), BF16),
            pltpu.VMEM((nev, loc), F32),
            pltpu.VMEM((2 * nev, loc), BF16),
            pltpu.VMEM((rows, width), F32),
            pltpu.VMEM((rows, width), BF16),
            pltpu.VMEM((rows, width), BF16),
            pltpu.VMEM((width, total), BF16),
            pltpu.VMEM((total, LANES), BF16),
            pltpu.VMEM((ndev,) + packed, F32),
            pltpu.VMEM((2 * rhs, total), BF16),
            pltpu.VMEM((ncol,) + packed, F32),
            pltpu.VMEM((ncol,) + packed, F32),
            pltpu.VMEM((ndev,) + packed, F32),
            pltpu.VMEM((4, rhs, BLK), F32),
            pltpu.VMEM((4, rhs, BLK), F32),
            dma((3,)),
            dma((4,)),
            dma((4,)),
            dma((4,)),
            dma((4,)),
            dma((ncol, nrow)),
            dma((ndev,)),
            dma((ncol,)),
            dma((ncol,)),
            dma((ncol, nrow)),
            dma((ndev,)),
        ],
        compiler_params=pltpu.CompilerParams(collective_id=0, has_side_effects=True),
    )(
        residuals.T,
        intersect_blocks,
        local_inverse,
        coarse_basis.T,
        coarse_slots.reshape(1, total),
        coarse_inverse,
    )
    return out.T


def solution(mesh):
    placed = (
        P(("row", "col"), None),
        P(("row", "col"), None),
        P(("row", "col"), None),
        P(("row", "col"), None),
        P(),
        P("row", "col"),
    )
    return jax.shard_map(
        functools.partial(shards, mesh.shape["row"], mesh.shape["col"]),
        mesh=mesh, in_specs=placed, out_specs=P(("row", "col"), None), check_vma=False,
    )
```

```python
import functools

import jax
import jax.numpy as jnp
from jax import lax
from jax.experimental import pallas as pl
from jax.experimental.pallas import tpu as pltpu
from jax.sharding import PartitionSpec as P

MESH = pl.DeviceIdType.MESH
BLK = 128
LANES = 128
UNROLL = 16
NT = (((1,), (1,)), ((), ()))
NN = (((1,), (0,)), ((), ()))
F32 = jnp.float32
BF16 = jnp.bfloat16


def matmul(a, b, dims):
    return lax.dot_general(a, b, dims, preferred_element_type=F32)


def split(x):
    hi = x.astype(BF16)
    return hi, (x - hi.astype(F32)).astype(BF16)


def loop(start, stop, body):
    if stop - start <= UNROLL:
        for i in range(start, stop):
            body(i)
    else:
        def step(i, carry):
            body(i)
            return carry

        lax.fori_loop(start, stop, step, 0)


def flipped(index, k, count):
    out = index
    bit = 1
    while bit < count:
        kbit = (k // bit) % 2
        out = out + kbit * bit * (1 - 2 * ((index // bit) % 2))
        bit *= 2
    return out


def lane_low(shape):
    return lax.broadcasted_iota(jnp.int32, shape, len(shape) - 1) < LANES // 2


def half_roll(x):
    return pltpu.roll(x, LANES // 2, 1)


def kernel(
    nrow,
    ncol,
    res_hbm,
    ib_hbm,
    linv_hbm,
    basis_hbm,
    slots_hbm,
    coarse_hbm,
    out_ref,
    res_ref,
    ib_ref,
    slots_ref,
    outgoing,
    incoming,
    linv,
    basis,
    basis2,
    coarse,
    coarse_hi,
    coarse_lo,
    hot_in,
    hot_out,
    gathered,
    gathered2,
    pieces,
    received,
    solved,
    lent,
    wide_hi,
    wide_lo,
    load_sem,
    halo_send,
    halo_recv,
    lend_send,
    lend_recv,
    ag1_send,
    ag1_recv,
    rs_send,
    rs_recv,
    ag2_send,
    ag2_recv,
):
    r = lax.axis_index("row")
    c = lax.axis_index("col")
    me = r * ncol + c
    rhs = res_ref.shape[0]
    own = res_ref.shape[1]
    half = rhs // 2
    ndev = nrow * ncol
    rows, width = coarse.shape
    total = slots_ref.shape[1]

    def col_peer(k):
        return (r, flipped(c, k, ncol))

    def row_peer(j):
        return (lax.rem(r + j, nrow), c)

    barrier = pltpu.get_barrier_semaphore()
    loop(1, ncol, lambda k: pl.semaphore_signal(barrier, inc=1, device_id=col_peer(ncol - k), device_id_type=MESH))
    loop(1, nrow, lambda j: pl.semaphore_signal(barrier, inc=1, device_id=row_peer(j), device_id_type=MESH))

    loads = [
        pltpu.make_async_copy(basis_hbm, basis, load_sem.at[0]),
        pltpu.make_async_copy(coarse_hbm, coarse, load_sem.at[1]),
        pltpu.make_async_copy(linv_hbm, linv, load_sem.at[2]),
        pltpu.make_async_copy(res_hbm, res_ref, load_sem.at[3]),
        pltpu.make_async_copy(ib_hbm, ib_ref, load_sem.at[4]),
        pltpu.make_async_copy(slots_hbm, slots_ref, load_sem.at[5]),
    ]
    for load in loads[3:] + loads[:3]:
        load.start()
    loads[4].wait()
    loads[3].wait()

    exists = [r < nrow - 1, r > 0, c < ncol - 1, c > 0]
    target = [(r + 1, c), (r - 1, c), (r, c + 1), (r, c - 1)]
    opposite = [1, 0, 3, 2]
    blocks = [res_ref[:, b * BLK:(b + 1) * BLK] for b in range(own // BLK)]
    for d in range(4):
        index = ib_ref[0, d]
        value = blocks[0]
        for b in range(1, len(blocks)):
            value = jnp.where(index == b, blocks[b], value)
        outgoing[d] = value

        @pl.when(jnp.logical_not(exists[opposite[d]]))
        def _():
            incoming[d] = jnp.zeros_like(incoming[d])

        @pl.when(jnp.logical_not(exists[d]))
        def _():
            lent[d] = jnp.zeros_like(lent[d])

    def halo(d):
        return pltpu.make_async_remote_copy(
            src_ref=outgoing.at[d], dst_ref=incoming.at[d],
            send_sem=halo_send.at[d], recv_sem=halo_recv.at[d],
            device_id=target[d], device_id_type=MESH)

    def lend(d):
        return pltpu.make_async_remote_copy(
            src_ref=basis.at[:, pl.ds(own + d * BLK, BLK)], dst_ref=lent.at[d],
            send_sem=lend_send.at[d], recv_sem=lend_recv.at[d],
            device_id=target[opposite[d]], device_id_type=MESH)

    pl.semaphore_wait(barrier, ncol + nrow - 2)
    for d in range(4):
        @pl.when(exists[d])
        def _():
            halo(d).start()

    loads[0].wait()
    nev = basis.shape[0]
    b_hi, b_lo = split(basis[...])
    basis2[:nev] = b_hi
    basis2[nev:] = b_lo
    partial = matmul(res_ref[...], basis2[:, :own], NT)

    for d in range(4):
        @pl.when(exists[opposite[d]])
        def _():
            halo(d).wait_recv()

    inc = jnp.concatenate([incoming[d] for d in range(4)], axis=1)
    partial = partial + matmul(inc, basis2[:, own:], NT)
    partial = partial + half_roll(partial)
    low = lane_low((half, LANES))
    gathered[me] = jnp.where(low, partial[:half], partial[half:])

    def spread(buf, send, recv):
        def to_col(k):
            return pltpu.make_async_remote_copy(
                src_ref=buf.at[me], dst_ref=buf.at[me],
                send_sem=send.at[k, 0], recv_sem=recv.at[me],
                device_id=col_peer(k), device_id_type=MESH)

        def to_row(k, j):
            slot = r * ncol + flipped(c, k, ncol)
            return pltpu.make_async_remote_copy(
                src_ref=buf.at[slot], dst_ref=buf.at[slot],
                send_sem=send.at[k, j], recv_sem=recv.at[slot],
                device_id=row_peer(j), device_id_type=MESH)

        def arrival(slot):
            pltpu.make_async_remote_copy(
                src_ref=buf.at[slot], dst_ref=buf.at[slot],
                send_sem=send.at[0, 0], recv_sem=recv.at[slot],
                device_id=row_peer(1), device_id_type=MESH).wait_recv()

        def start():
            loop(1, ncol, lambda i: to_col(ncol - i).start())
            for j in range(1, nrow):
                to_row(0, j).start()

        def relay(first, last):
            def one(k):
                arrival(r * ncol + flipped(c, k, ncol))
                for j in range(1, nrow):
                    to_row(k, j).start()

            loop(first, last, one)

        def finish():
            def one(k):
                for j in range(1, nrow):
                    arrival(lax.rem(r + j, nrow) * ncol + flipped(c, k, ncol))

            loop(0, ncol, one)

        def drain():
            def one(k):
                for j in range(1, nrow):
                    to_row(k, j).wait_send()

            loop(0, ncol, one)
            loop(1, ncol, lambda k: to_col(k).wait_send())

        return start, relay, finish, drain

    def unpacked(buf):
        def one(p):
            a, b = buf[2 * p], buf[2 * p + 1]
            top = jnp.where(low, a, half_roll(b))
            bot = jnp.where(low, half_roll(a), b)
            t_hi, t_lo = split(top)
            b_hi, b_lo = split(bot)
            lanes = pl.ds(p * LANES if isinstance(p, int) else pl.multiple_of(p * LANES, LANES), LANES)
            gathered2[0 * half:1 * half, lanes] = t_hi
            gathered2[1 * half:2 * half, lanes] = b_hi
            gathered2[2 * half:3 * half, lanes] = t_lo
            gathered2[3 * half:4 * half, lanes] = b_lo

        loop(0, ndev // 2, one)

    start1, relay1, finish1, drain1 = spread(gathered, ag1_send, ag1_recv)
    start1()
    for d in range(4):
        @pl.when(exists[opposite[d]])
        def _():
            lend(d).start()

    loads[2].wait()
    local = jnp.concatenate([res_ref[...], inc], axis=1)
    out_ref[...] = matmul(local, linv[...], NT)
    relay1(1, ncol // 2)
    chunk = 2 * LANES
    loads[5].wait()

    def build_in(i):
        lanes = pl.ds(i * chunk if isinstance(i, int) else pl.multiple_of(i * chunk, chunk), chunk)
        slot = slots_ref[:, lanes] - c * width
        place = lax.broadcasted_iota(jnp.int32, (width, chunk), 0)
        hot_in[:, lanes] = jnp.where(place == slot, 1.0, 0.0).astype(BF16)

    loop(0, total // chunk, build_in)
    relay1(ncol // 2, ncol)
    loads[1].wait()
    a_hi, a_lo = split(coarse[...])
    coarse_hi[...] = a_hi
    coarse_lo[...] = a_lo
    finish1()

    unpacked(gathered)
    depth = min(total, 2048)
    column = matmul(gathered2[:, :depth], hot_in[:, :depth], NT)
    if total > depth:
        def more(i, acc):
            lanes = pl.ds(pl.multiple_of(i * depth, depth), depth)
            return acc + matmul(gathered2[:, lanes], hot_in[:, lanes], NT)

        column = lax.fori_loop(1, total // depth, more, column)
    column_hi, column_lo = split(column[:rhs] + column[rhs:])
    column2 = jnp.concatenate([column_hi, column_lo], axis=0)
    span = 2 * LANES

    def product(i):
        at = pl.ds(i * span if isinstance(i, int) else pl.multiple_of(i * span, span), span)
        part = matmul(column2, coarse_hi[at], NT) + matmul(column2, coarse_lo[at], NT)
        part = part[:rhs] + part[rhs:]
        for q in range(span // LANES):
            top = part[:half, q * LANES:(q + 1) * LANES]
            bot = part[half:, q * LANES:(q + 1) * LANES]
            pieces[(span // LANES * i + q) * 2] = jnp.where(low, top, half_roll(bot))
            pieces[(span // LANES * i + q) * 2 + 1] = jnp.where(low, half_roll(top), bot)

    loop(0, rows // span, product)

    def reduce(k):
        peer = flipped(c, k, ncol)
        return pltpu.make_async_remote_copy(
            src_ref=pieces.at[peer], dst_ref=received.at[c],
            send_sem=rs_send.at[k], recv_sem=rs_recv.at[c],
            device_id=(r, peer), device_id_type=MESH)

    def reduce_arrival(k):
        peer = flipped(c, k, ncol)
        pltpu.make_async_remote_copy(
            src_ref=pieces.at[peer], dst_ref=received.at[peer],
            send_sem=rs_send.at[k], recv_sem=rs_recv.at[peer],
            device_id=(r, peer), device_id_type=MESH).wait_recv()

    loop(1, ncol, lambda i: reduce(ncol - i).start())

    low8 = lane_low((8, LANES))

    def slots_of(device):
        device = jnp.clip(device, 0, ndev - 1)
        at = pl.ds(pl.multiple_of((device // 2) * LANES, LANES), LANES)
        pair = jnp.broadcast_to(slots_ref[:, at], (8, LANES))
        swapped = half_roll(pair)
        return jnp.where(lax.rem(device, 2) == 0, jnp.where(low8, pair, swapped), jnp.where(low8, swapped, pair))

    mine = [
        jnp.where(low8, slots_of(me), slots_of(me + ncol))[:1],
        jnp.where(low8, slots_of(me - ncol), slots_of(me + 1))[:1],
        jnp.where(low8, slots_of(me - 1), -1)[:1],
    ]
    tall = 4 * LANES

    def build_out(i):
        at = pl.ds(i * tall if isinstance(i, int) else pl.multiple_of(i * tall, tall), tall)
        place = lax.broadcasted_iota(jnp.int32, (tall, LANES), 0) + i * tall
        for q in range(3):
            hot_out[at, q * LANES:(q + 1) * LANES] = jnp.where(place == mine[q], 1.0, 0.0).astype(BF16)

    loop(0, total // tall, build_out)

    wide_hi[:nev] = basis2[:nev, :own]
    wide_lo[:nev] = basis2[nev:, :own]
    wide_hi[5 * nev:] = jnp.zeros_like(wide_hi[5 * nev:])
    wide_lo[5 * nev:] = jnp.zeros_like(wide_lo[5 * nev:])
    for d in range(4):
        @pl.when(exists[d])
        def _():
            lend(d).wait_recv()

        l_hi, l_lo = split(lent[d])
        for b in range(own // BLK):
            here = ib_ref[0, d] == b
            at = slice((d + 1) * nev, (d + 2) * nev), slice(b * BLK, (b + 1) * BLK)
            wide_hi[at] = jnp.where(here, l_hi, jnp.zeros_like(l_hi))
            wide_lo[at] = jnp.where(here, l_lo, jnp.zeros_like(l_lo))

    loop(1, ncol, reduce_arrival)
    summed = pieces[c]
    if ncol - 1 <= UNROLL:
        for k in range(1, ncol):
            summed = summed + received[flipped(c, k, ncol)]
    else:
        summed = lax.fori_loop(1, ncol, lambda k, acc: acc + received[flipped(c, k, ncol)], summed)
    solved[me] = summed

    start2, relay2, finish2, drain2 = spread(solved, ag2_send, ag2_recv)
    start2()
    relay2(1, ncol)
    finish2()
    unpacked(solved)
    picked = matmul(gathered2[:, :depth], hot_out[:depth], NN)
    if total > depth:
        def again(i, acc):
            at = pl.ds(pl.multiple_of(i * depth, depth), depth)
            return acc + matmul(gathered2[:, at], hot_out[at], NN)

        picked = lax.fori_loop(1, total // depth, again, picked)
    picked = picked.astype(BF16)

    inner = matmul(picked, wide_hi[...], NN) + matmul(picked, wide_lo[...], NN)
    out_ref[...] = out_ref[...] + inner[:rhs] + inner[rhs:]

    drain1()
    drain2()
    loop(1, ncol, lambda k: reduce(k).wait_send())
    for d in range(4):
        @pl.when(exists[d])
        def _():
            halo(d).wait_send()

        @pl.when(exists[opposite[d]])
        def _():
            lend(d).wait_send()


def shards(nrow, ncol, residuals, intersect_blocks, local_inverse, coarse_basis, coarse_slots, coarse_inverse):
    own, rhs = residuals.shape
    loc, nev = coarse_basis.shape
    rows, width = coarse_inverse.shape
    total = coarse_slots.shape[0]
    ndev = nrow * ncol
    assert 2 * nev == LANES and rows == ncol * nev and loc == own + 4 * BLK and own % BLK == 0
    packed = (rhs // 2, LANES)
    vmem = pl.BlockSpec(memory_space=pltpu.VMEM)
    hbm = pl.BlockSpec(memory_space=pl.ANY)
    dma = pltpu.SemaphoreType.DMA
    out = pl.pallas_call(
        functools.partial(kernel, nrow, ncol),
        name="schwarz",
        out_shape=pltpu.VMEM((rhs, own), F32),
        in_specs=[hbm] * 6,
        out_specs=vmem,
        scratch_shapes=[
            pltpu.VMEM((rhs, own), BF16),
            pltpu.SMEM(intersect_blocks.shape, jnp.int32),
            pltpu.VMEM((1, total), jnp.int32),
            pltpu.VMEM((4, rhs, BLK), BF16),
            pltpu.VMEM((4, rhs, BLK), BF16),
            pltpu.VMEM((own, loc), BF16),
            pltpu.VMEM((nev, loc), F32),
            pltpu.VMEM((2 * nev, loc), BF16),
            pltpu.VMEM((rows, width), F32),
            pltpu.VMEM((rows, width), BF16),
            pltpu.VMEM((rows, width), BF16),
            pltpu.VMEM((width, total), BF16),
            pltpu.VMEM((total, 3 * LANES), BF16),
            pltpu.VMEM((ndev,) + packed, F32),
            pltpu.VMEM((2 * rhs, total), BF16),
            pltpu.VMEM((ncol,) + packed, F32),
            pltpu.VMEM((ncol,) + packed, F32),
            pltpu.VMEM((ndev,) + packed, F32),
            pltpu.VMEM((4, nev, BLK), F32),
            pltpu.VMEM((6 * nev, own), BF16),
            pltpu.VMEM((6 * nev, own), BF16),
            dma((6,)),
            dma((4,)),
            dma((4,)),
            dma((4,)),
            dma((4,)),
            dma((ncol, nrow)),
            dma((ndev,)),
            dma((ncol,)),
            dma((ncol,)),
            dma((ncol, nrow)),
            dma((ndev,)),
        ],
        compiler_params=pltpu.CompilerParams(collective_id=0, has_side_effects=True),
    )(
        residuals.T,
        intersect_blocks,
        local_inverse,
        coarse_basis.T,
        coarse_slots.reshape(1, total),
        coarse_inverse,
    )
    return out.T


def solution(mesh):
    placed = (
        P(("row", "col"), None),
        P(("row", "col"), None),
        P(("row", "col"), None),
        P(("row", "col"), None),
        P(),
        P("row", "col"),
    )
    return jax.shard_map(
        functools.partial(shards, mesh.shape["row"], mesh.shape["col"]),
        mesh=mesh, in_specs=placed, out_specs=P(("row", "col"), None), check_vma=False,
    )
```

```python
import functools

import jax
import jax.numpy as jnp
from jax import lax
from jax.experimental import pallas as pl
from jax.experimental.pallas import tpu as pltpu
from jax.sharding import PartitionSpec as P

MESH = pl.DeviceIdType.MESH
BLK = 128
LANES = 128
UNROLL = 16
FAR_NUM, FAR_DEN = 3, 4
NT = (((1,), (1,)), ((), ()))
NN = (((1,), (0,)), ((), ()))
F32 = jnp.float32
BF16 = jnp.bfloat16


def matmul(a, b, dims):
    return lax.dot_general(a, b, dims, preferred_element_type=F32)


def split(x):
    hi = x.astype(BF16)
    return hi, (x - hi.astype(F32)).astype(BF16)


def loop(start, stop, body):
    if stop - start <= UNROLL:
        for i in range(start, stop):
            body(i)
    else:
        def step(i, carry):
            body(i)
            return carry

        lax.fori_loop(start, stop, step, 0)


def flipped(index, k, count):
    out = index
    bit = 1
    while bit < count:
        kbit = (k // bit) % 2
        out = out + kbit * bit * (1 - 2 * ((index // bit) % 2))
        bit *= 2
    return out


def lane_low(shape):
    return lax.broadcasted_iota(jnp.int32, shape, len(shape) - 1) < LANES // 2


def half_roll(x):
    return pltpu.roll(x, LANES // 2, 1)


def kernel(
    nrow,
    ncol,
    res_hbm,
    ib_hbm,
    linv_hbm,
    basis_hbm,
    slots_hbm,
    coarse_hbm,
    out_ref,
    res_ref,
    ib_ref,
    slots_ref,
    outgoing,
    incoming,
    linv,
    basis,
    basis2,
    coarse,
    coarse_hi,
    coarse_lo,
    hot_in,
    hot_out,
    gathered,
    gathered2,
    pieces,
    received,
    solved,
    lent,
    wide_hi,
    wide_lo,
    load_sem,
    halo_send,
    halo_recv,
    lend_send,
    lend_recv,
    ag1_send,
    ag1_recv,
    ag1_rest,
    rs_send,
    rs_recv,
    ag2_send,
    ag2_recv,
    ag2_rest,
):
    r = lax.axis_index("row")
    c = lax.axis_index("col")
    me = r * ncol + c
    rhs = res_ref.shape[0]
    own = res_ref.shape[1]
    half = rhs // 2
    ndev = nrow * ncol
    rows, width = coarse.shape
    total = slots_ref.shape[1]

    def col_peer(k):
        return (r, flipped(c, k, ncol))

    def row_peer(j):
        return (lax.rem(r + j, nrow), c)

    barrier = pltpu.get_barrier_semaphore()
    loop(1, ncol, lambda k: pl.semaphore_signal(barrier, inc=1, device_id=col_peer(ncol - k), device_id_type=MESH))
    loop(1, nrow, lambda j: pl.semaphore_signal(barrier, inc=1, device_id=row_peer(j), device_id_type=MESH))

    loads = [
        pltpu.make_async_copy(basis_hbm, basis, load_sem.at[0]),
        pltpu.make_async_copy(coarse_hbm, coarse, load_sem.at[1]),
        pltpu.make_async_copy(linv_hbm, linv, load_sem.at[2]),
        pltpu.make_async_copy(res_hbm, res_ref, load_sem.at[3]),
        pltpu.make_async_copy(ib_hbm, ib_ref, load_sem.at[4]),
        pltpu.make_async_copy(slots_hbm, slots_ref, load_sem.at[5]),
    ]
    for load in loads[3:] + loads[:3]:
        load.start()
    loads[4].wait()
    loads[3].wait()

    exists = [r < nrow - 1, r > 0, c < ncol - 1, c > 0]
    target = [(r + 1, c), (r - 1, c), (r, c + 1), (r, c - 1)]
    opposite = [1, 0, 3, 2]
    blocks = [res_ref[:, b * BLK:(b + 1) * BLK] for b in range(own // BLK)]
    for d in range(4):
        index = ib_ref[0, d]
        value = blocks[0]
        for b in range(1, len(blocks)):
            value = jnp.where(index == b, blocks[b], value)
        outgoing[d] = value

        @pl.when(jnp.logical_not(exists[opposite[d]]))
        def _():
            incoming[d] = jnp.zeros_like(incoming[d])

        @pl.when(jnp.logical_not(exists[d]))
        def _():
            lent[d] = jnp.zeros_like(lent[d])

    def halo(d):
        return pltpu.make_async_remote_copy(
            src_ref=outgoing.at[d], dst_ref=incoming.at[d],
            send_sem=halo_send.at[d], recv_sem=halo_recv.at[d],
            device_id=target[d], device_id_type=MESH)

    def lend(d):
        return pltpu.make_async_remote_copy(
            src_ref=basis.at[:, pl.ds(own + d * BLK, BLK)], dst_ref=lent.at[d],
            send_sem=lend_send.at[d], recv_sem=lend_recv.at[d],
            device_id=target[opposite[d]], device_id_type=MESH)

    pl.semaphore_wait(barrier, ncol + nrow - 2)
    for d in range(4):
        @pl.when(exists[d])
        def _():
            halo(d).start()

    loads[0].wait()
    nev = basis.shape[0]
    b_hi, b_lo = split(basis[...])
    basis2[:nev] = b_hi
    basis2[nev:] = b_lo
    partial = matmul(res_ref[...], basis2[:, :own], NT)

    for d in range(4):
        @pl.when(exists[opposite[d]])
        def _():
            halo(d).wait_recv()

    inc = jnp.concatenate([incoming[d] for d in range(4)], axis=1)
    partial = partial + matmul(inc, basis2[:, own:], NT)
    partial = partial + half_roll(partial)
    low = lane_low((half, LANES))
    gathered[me] = jnp.where(low, partial[:half], partial[half:])

    def spread(buf, send, recv, rest, far):
        pairs = nrow // 2
        partner = r + 1 - 2 * lax.rem(r, 2)
        singles = ncol - 1 + (pairs - 1) * (ncol - far)

        def copy(slot, sem, device):
            return pltpu.make_async_remote_copy(
                src_ref=buf.at[slot], dst_ref=buf.at[slot], send_sem=send.at[0], recv_sem=sem,
                device_id=device, device_id_type=MESH)

        def pair_row(q):
            return lax.rem(r + 2 * q, nrow)

        def start():
            def one(i):
                k = ncol - i
                for q in range(pairs if i <= ncol - far else 1):
                    copy(me, recv.at[k, q], (pair_row(q), flipped(c, k, ncol))).start()

            if far == ncol:
                loop(1, ncol, lambda i: copy(me, recv.at[ncol - i, 0], col_peer(ncol - i)).start())
            else:
                for i in range(1, ncol):
                    one(i)
            share(r * ncol + c)

        def share(slot):
            for q in range(1, pairs):
                copy(slot, rest.at[0], (pair_row(q), c)).start()
            for q in range(1, pairs):
                copy(slot, rest.at[0], (lax.rem(partner + 2 * q, nrow), c)).start()
            copy(slot, rest.at[0], (partner, c)).start()

        def arrival(slot, k, q):
            copy(slot, recv.at[k, q], (partner, c)).wait_recv()

        def relay(first, last):
            def near(k):
                slot = r * ncol + flipped(c, k, ncol)
                arrival(slot, k, 0)
                share(slot)

            def distant(k):
                for q in range(pairs):
                    slot = pair_row(pairs - q) * ncol + flipped(c, k, ncol)
                    arrival(slot, k, q)
                    copy(slot, rest.at[0], (partner, c)).start()

            loop(first, min(last, far), near)
            if last > far:
                loop(max(first, far), last, distant)

        def finish():
            some = buf.at[pl.ds(0, ndev - 1 - singles)]
            pltpu.make_async_copy(some, some, rest.at[0]).wait()

        def drain():
            count = singles + far * (nrow - 1) + (ncol - far) * pairs
            while count > 0:
                now = min(count, ndev)
                some = buf.at[pl.ds(0, now)]
                pltpu.make_async_copy(some, some, send.at[0]).wait()
                count -= now

        return start, relay, finish, drain

    def unpacked(buf):
        def one(p):
            a, b = buf[2 * p], buf[2 * p + 1]
            top = jnp.where(low, a, half_roll(b))
            bot = jnp.where(low, half_roll(a), b)
            t_hi, t_lo = split(top)
            b_hi, b_lo = split(bot)
            lanes = pl.ds(p * LANES if isinstance(p, int) else pl.multiple_of(p * LANES, LANES), LANES)
            gathered2[0 * half:1 * half, lanes] = t_hi
            gathered2[1 * half:2 * half, lanes] = b_hi
            gathered2[2 * half:3 * half, lanes] = t_lo
            gathered2[3 * half:4 * half, lanes] = b_lo

        loop(0, ndev // 2, one)

    start1, relay1, finish1, drain1 = spread(gathered, ag1_send, ag1_recv, ag1_rest, ncol)
    start1()

    loads[2].wait()
    local = jnp.concatenate([res_ref[...], inc], axis=1)
    out_ref[...] = matmul(local, linv[...], NT)
    relay1(1, ncol // 2)
    chunk = 2 * LANES
    loads[5].wait()

    def build_in(i):
        lanes = pl.ds(i * chunk if isinstance(i, int) else pl.multiple_of(i * chunk, chunk), chunk)
        slot = slots_ref[:, lanes] - c * width
        place = lax.broadcasted_iota(jnp.int32, (width, chunk), 0)
        hot_in[:, lanes] = jnp.where(place == slot, 1.0, 0.0).astype(BF16)

    loop(0, total // chunk, build_in)
    relay1(ncol // 2, ncol)
    loads[1].wait()
    a_hi, a_lo = split(coarse[...])
    coarse_hi[...] = a_hi
    coarse_lo[...] = a_lo
    finish1()
    for d in range(4):
        @pl.when(exists[opposite[d]])
        def _():
            lend(d).start()

    unpacked(gathered)
    depth = min(total, 2048)
    column = matmul(gathered2[:, :depth], hot_in[:, :depth], NT)
    if total > depth:
        def more(i, acc):
            lanes = pl.ds(pl.multiple_of(i * depth, depth), depth)
            return acc + matmul(gathered2[:, lanes], hot_in[:, lanes], NT)

        column = lax.fori_loop(1, total // depth, more, column)
    column_hi, column_lo = split(column[:rhs] + column[rhs:])
    column2 = jnp.concatenate([column_hi, column_lo], axis=0)
    span = 2 * LANES

    def product(i):
        at = pl.ds(i * span if isinstance(i, int) else pl.multiple_of(i * span, span), span)
        part = matmul(column2, coarse_hi[at], NT) + matmul(column2, coarse_lo[at], NT)
        part = part[:rhs] + part[rhs:]
        for q in range(span // LANES):
            top = part[:half, q * LANES:(q + 1) * LANES]
            bot = part[half:, q * LANES:(q + 1) * LANES]
            pieces[(span // LANES * i + q) * 2] = jnp.where(low, top, half_roll(bot))
            pieces[(span // LANES * i + q) * 2 + 1] = jnp.where(low, half_roll(top), bot)

    loop(0, rows // span, product)

    def reduce(k):
        peer = flipped(c, k, ncol)
        return pltpu.make_async_remote_copy(
            src_ref=pieces.at[peer], dst_ref=received.at[c],
            send_sem=rs_send.at[0], recv_sem=rs_recv.at[0],
            device_id=(r, peer), device_id_type=MESH)

    loop(1, ncol, lambda i: reduce(ncol - i).start())

    low8 = lane_low((8, LANES))

    def slots_of(device):
        device = jnp.clip(device, 0, ndev - 1)
        at = pl.ds(pl.multiple_of((device // 2) * LANES, LANES), LANES)
        pair = jnp.broadcast_to(slots_ref[:, at], (8, LANES))
        swapped = half_roll(pair)
        return jnp.where(lax.rem(device, 2) == 0, jnp.where(low8, pair, swapped), jnp.where(low8, swapped, pair))

    mine = [
        jnp.where(low8, slots_of(me), slots_of(me + ncol))[:1],
        jnp.where(low8, slots_of(me - ncol), slots_of(me + 1))[:1],
        jnp.where(low8, slots_of(me - 1), -1)[:1],
    ]
    tall = 4 * LANES

    def build_out(i):
        at = pl.ds(i * tall if isinstance(i, int) else pl.multiple_of(i * tall, tall), tall)
        place = lax.broadcasted_iota(jnp.int32, (tall, LANES), 0) + i * tall
        for q in range(3):
            hot_out[at, q * LANES:(q + 1) * LANES] = jnp.where(place == mine[q], 1.0, 0.0).astype(BF16)

    loop(0, total // tall, build_out)

    wide_hi[:nev] = basis2[:nev, :own]
    wide_lo[:nev] = basis2[nev:, :own]
    wide_hi[5 * nev:] = jnp.zeros_like(wide_hi[5 * nev:])
    wide_lo[5 * nev:] = jnp.zeros_like(wide_lo[5 * nev:])
    for d in range(4):
        @pl.when(exists[d])
        def _():
            lend(d).wait_recv()

        l_hi, l_lo = split(lent[d])
        for b in range(own // BLK):
            here = ib_ref[0, d] == b
            at = slice((d + 1) * nev, (d + 2) * nev), slice(b * BLK, (b + 1) * BLK)
            wide_hi[at] = jnp.where(here, l_hi, jnp.zeros_like(l_hi))
            wide_lo[at] = jnp.where(here, l_lo, jnp.zeros_like(l_lo))

    others = received.at[pl.ds(0, ncol - 1)]
    pltpu.make_async_copy(others, others, rs_recv.at[0]).wait()
    summed = pieces[c]
    if ncol - 1 <= UNROLL:
        for k in range(1, ncol):
            summed = summed + received[flipped(c, k, ncol)]
    else:
        summed = lax.fori_loop(1, ncol, lambda k, acc: acc + received[flipped(c, k, ncol)], summed)
    solved[me] = summed

    start2, relay2, finish2, drain2 = spread(solved, ag2_send, ag2_recv, ag2_rest, ncol * FAR_NUM // FAR_DEN)
    start2()
    relay2(1, ncol)
    finish2()
    unpacked(solved)
    picked = matmul(gathered2[:, :depth], hot_out[:depth], NN)
    if total > depth:
        def again(i, acc):
            at = pl.ds(pl.multiple_of(i * depth, depth), depth)
            return acc + matmul(gathered2[:, at], hot_out[at], NN)

        picked = lax.fori_loop(1, total // depth, again, picked)
    picked = picked.astype(BF16)

    inner = matmul(picked, wide_hi[...], NN) + matmul(picked, wide_lo[...], NN)
    out_ref[...] = out_ref[...] + inner[:rhs] + inner[rhs:]

    drain1()
    drain2()
    pltpu.make_async_copy(others, others, rs_send.at[0]).wait()
    for d in range(4):
        @pl.when(exists[d])
        def _():
            halo(d).wait_send()

        @pl.when(exists[opposite[d]])
        def _():
            lend(d).wait_send()


def shards(nrow, ncol, residuals, intersect_blocks, local_inverse, coarse_basis, coarse_slots, coarse_inverse):
    own, rhs = residuals.shape
    loc, nev = coarse_basis.shape
    rows, width = coarse_inverse.shape
    total = coarse_slots.shape[0]
    ndev = nrow * ncol
    assert 2 * nev == LANES and rows == ncol * nev and loc == own + 4 * BLK and own % BLK == 0
    packed = (rhs // 2, LANES)
    vmem = pl.BlockSpec(memory_space=pltpu.VMEM)
    hbm = pl.BlockSpec(memory_space=pl.ANY)
    dma = pltpu.SemaphoreType.DMA
    out = pl.pallas_call(
        functools.partial(kernel, nrow, ncol),
        name="schwarz",
        out_shape=pltpu.VMEM((rhs, own), F32),
        in_specs=[hbm] * 6,
        out_specs=vmem,
        scratch_shapes=[
            pltpu.VMEM((rhs, own), BF16),
            pltpu.SMEM(intersect_blocks.shape, jnp.int32),
            pltpu.VMEM((1, total), jnp.int32),
            pltpu.VMEM((4, rhs, BLK), BF16),
            pltpu.VMEM((4, rhs, BLK), BF16),
            pltpu.VMEM((own, loc), BF16),
            pltpu.VMEM((nev, loc), F32),
            pltpu.VMEM((2 * nev, loc), BF16),
            pltpu.VMEM((rows, width), F32),
            pltpu.VMEM((rows, width), BF16),
            pltpu.VMEM((rows, width), BF16),
            pltpu.VMEM((width, total), BF16),
            pltpu.VMEM((total, 3 * LANES), BF16),
            pltpu.VMEM((ndev,) + packed, F32),
            pltpu.VMEM((2 * rhs, total), BF16),
            pltpu.VMEM((ncol,) + packed, F32),
            pltpu.VMEM((ncol,) + packed, F32),
            pltpu.VMEM((ndev,) + packed, F32),
            pltpu.VMEM((4, nev, BLK), F32),
            pltpu.VMEM((6 * nev, own), BF16),
            pltpu.VMEM((6 * nev, own), BF16),
            dma((6,)),
            dma((4,)),
            dma((4,)),
            dma((4,)),
            dma((4,)),
            dma((1,)),
            dma((ncol, 1)),
            dma((1,)),
            dma((1,)),
            dma((1,)),
            dma((1,)),
            dma((ncol, nrow // 2)),
            dma((1,)),
        ],
        compiler_params=pltpu.CompilerParams(collective_id=0, has_side_effects=True),
    )(
        residuals.T,
        intersect_blocks,
        local_inverse,
        coarse_basis.T,
        coarse_slots.reshape(1, total),
        coarse_inverse,
    )
    return out.T


def solution(mesh):
    placed = (
        P(("row", "col"), None),
        P(("row", "col"), None),
        P(("row", "col"), None),
        P(("row", "col"), None),
        P(),
        P("row", "col"),
    )
    return jax.shard_map(
        functools.partial(shards, mesh.shape["row"], mesh.shape["col"]),
        mesh=mesh, in_specs=placed, out_specs=P(("row", "col"), None), check_vma=False,
    )
```

```python
import functools

import jax
import jax.numpy as jnp
from jax import lax
from jax.experimental import pallas as pl
from jax.experimental.pallas import tpu as pltpu
from jax.sharding import PartitionSpec as P

MESH = pl.DeviceIdType.MESH
BLK = 128
LANES = 128
UNROLL = 16
FAR_NUM, FAR_DEN = 1, 2
NT = (((1,), (1,)), ((), ()))
NN = (((1,), (0,)), ((), ()))
F32 = jnp.float32
BF16 = jnp.bfloat16


def matmul(a, b, dims):
    return lax.dot_general(a, b, dims, preferred_element_type=F32)


def split(x):
    hi = x.astype(BF16)
    return hi, (x - hi.astype(F32)).astype(BF16)


def loop(start, stop, body):
    if stop - start <= UNROLL:
        for i in range(start, stop):
            body(i)
    else:
        def step(i, carry):
            body(i)
            return carry

        lax.fori_loop(start, stop, step, 0)


def flipped(index, k, count):
    out = index
    bit = 1
    while bit < count:
        kbit = (k // bit) % 2
        out = out + kbit * bit * (1 - 2 * ((index // bit) % 2))
        bit *= 2
    return out


def lane_low(shape):
    return lax.broadcasted_iota(jnp.int32, shape, len(shape) - 1) < LANES // 2


def half_roll(x):
    return pltpu.roll(x, LANES // 2, 1)


def kernel(
    nrow,
    ncol,
    res_hbm,
    ib_hbm,
    linv_hbm,
    basis_hbm,
    slots_hbm,
    coarse_hbm,
    out_ref,
    res_ref,
    ib_ref,
    slots_ref,
    outgoing,
    incoming,
    linv,
    basis,
    basis2,
    coarse,
    coarse_hi,
    coarse_lo,
    hot_in,
    hot_out,
    gathered,
    pieces,
    received,
    solved,
    lent,
    wide_hi,
    wide_lo,
    passed,
    load_sem,
    halo_send,
    halo_recv,
    lend_send,
    lend_recv,
    ag1_send,
    ag1_recv,
    ag1_rest,
    rs_send,
    rs_recv,
    ag2_send,
    ag2_recv,
    ag2_rest,
):
    r = lax.axis_index("row")
    c = lax.axis_index("col")
    me = r * ncol + c
    rhs = res_ref.shape[0]
    own = res_ref.shape[1]
    half = rhs // 2
    ndev = nrow * ncol
    rows, width = coarse.shape
    total = slots_ref.shape[1]

    near = ncol * FAR_NUM // FAR_DEN

    def col_peer(k):
        return (r, flipped(c, k, ncol))

    def row_peer(j):
        return (lax.rem(r + j, nrow), c)

    barrier = pltpu.get_barrier_semaphore()
    loop(1, ncol, lambda k: pl.semaphore_signal(barrier, inc=1, device_id=col_peer(ncol - k), device_id_type=MESH))
    loop(1, nrow, lambda j: pl.semaphore_signal(barrier, inc=1, device_id=row_peer(j), device_id_type=MESH))

    loads = [
        pltpu.make_async_copy(basis_hbm, basis, load_sem.at[0]),
        pltpu.make_async_copy(coarse_hbm, coarse, load_sem.at[1]),
        pltpu.make_async_copy(linv_hbm, linv, load_sem.at[2]),
        pltpu.make_async_copy(res_hbm, res_ref, load_sem.at[3]),
        pltpu.make_async_copy(ib_hbm, ib_ref, load_sem.at[4]),
        pltpu.make_async_copy(slots_hbm, slots_ref, load_sem.at[5]),
    ]
    for load in loads[3:] + loads[:3]:
        load.start()
    loads[4].wait()
    loads[3].wait()

    exists = [r < nrow - 1, r > 0, c < ncol - 1, c > 0]
    target = [(r + 1, c), (r - 1, c), (r, c + 1), (r, c - 1)]
    opposite = [1, 0, 3, 2]
    blocks = [res_ref[:, b * BLK:(b + 1) * BLK] for b in range(own // BLK)]
    for d in range(4):
        index = ib_ref[0, d]
        value = blocks[0]
        for b in range(1, len(blocks)):
            value = jnp.where(index == b, blocks[b], value)
        outgoing[d] = value

        @pl.when(jnp.logical_not(exists[opposite[d]]))
        def _():
            incoming[d] = jnp.zeros_like(incoming[d])

        @pl.when(jnp.logical_not(exists[d]))
        def _():
            lent[d] = jnp.zeros_like(lent[d])

    def halo(d):
        return pltpu.make_async_remote_copy(
            src_ref=outgoing.at[d], dst_ref=incoming.at[d],
            send_sem=halo_send.at[d], recv_sem=halo_recv.at[d],
            device_id=target[d], device_id_type=MESH)

    def lend(d):
        return pltpu.make_async_remote_copy(
            src_ref=basis.at[:, pl.ds(own + d * BLK, BLK)], dst_ref=lent.at[d],
            send_sem=lend_send.at[d], recv_sem=lend_recv.at[d],
            device_id=target[opposite[d]], device_id_type=MESH)

    pl.semaphore_wait(barrier, ncol + nrow - 2)
    for q in range(1, nrow // 2):
        pl.semaphore_signal(passed, inc=1, device_id=(lax.rem(r + 2 * q, nrow), c), device_id_type=MESH)
    for d in range(4):
        @pl.when(exists[d])
        def _():
            halo(d).start()

    loads[0].wait()
    nev = basis.shape[0]
    b_hi, b_lo = split(basis[...])
    basis2[:nev] = b_hi
    basis2[nev:] = b_lo
    partial = matmul(res_ref[...], basis2[:, :own], NT)

    for d in range(4):
        @pl.when(exists[opposite[d]])
        def _():
            halo(d).wait_recv()

    inc = jnp.concatenate([incoming[d] for d in range(4)], axis=1)
    partial = partial + matmul(inc, basis2[:, own:], NT)
    partial = partial + half_roll(partial)
    low = lane_low((half, LANES))
    gathered[me] = jnp.where(low, partial[:half], partial[half:])

    def spread(buf, send, recv, rest, far):
        pairs = nrow // 2
        partner = r + 1 - 2 * lax.rem(r, 2)
        singles = ncol - 1 + (pairs - 1) * (ncol - far)

        def copy(slot, sem, device):
            return pltpu.make_async_remote_copy(
                src_ref=buf.at[slot], dst_ref=buf.at[slot], send_sem=send.at[0], recv_sem=sem,
                device_id=device, device_id_type=MESH)

        def pair_row(q):
            return lax.rem(r + 2 * q, nrow)

        def start():
            def one(i):
                k = ncol - i
                for q in range(pairs if i <= ncol - far else 1):
                    copy(me, recv.at[k, q], (pair_row(q), flipped(c, k, ncol))).start()

            if far == ncol:
                loop(1, ncol, lambda i: copy(me, recv.at[ncol - i, 0], col_peer(ncol - i)).start())
            else:
                for i in range(1, ncol):
                    one(i)
            share(r * ncol + c)

        def share(slot):
            for q in range(1, pairs):
                copy(slot, rest.at[pairs - q], (pair_row(q), c)).start()
            for q in range(1, pairs):
                copy(slot, rest.at[2 * pairs - q], (lax.rem(partner + 2 * q, nrow), c)).start()
            copy(slot, rest.at[pairs], (partner, c)).start()

        def arrival(slot, k, q):
            copy(slot, recv.at[k, q], (partner, c)).wait_recv()

        def relay(first, last):
            def near(k):
                slot = r * ncol + flipped(c, k, ncol)
                arrival(slot, k, 0)
                share(slot)

            def distant(k):
                for q in range(pairs):
                    slot = pair_row(pairs - q) * ncol + flipped(c, k, ncol)
                    arrival(slot, k, q)
                    copy(slot, rest.at[pairs + (pairs - q) % pairs], (partner, c)).start()

            loop(first, min(last, far), near)
            if last > far:
                loop(max(first, far), last, distant)

        def finish(consume):
            def wait(index, count):
                some = buf.at[pl.ds(0, count)]
                pltpu.make_async_copy(some, some, rest.at[index]).wait()

            total = consume(r, None)
            wait(pairs, ncol)
            total = consume(partner, total)
            for o in range(1, pairs):
                wait(o, far)
                total = consume(pair_row(o), total)
            for o in range(1, pairs):
                wait(pairs + o, ncol)
                total = consume(lax.rem(partner + 2 * o, nrow), total)
            return total

        def drain():
            count = singles + far * (nrow - 1) + (ncol - far) * pairs
            while count > 0:
                now = min(count, ndev)
                some = buf.at[pl.ds(0, now)]
                pltpu.make_async_copy(some, some, send.at[0]).wait()
                count -= now

        return start, relay, finish, drain

    depth = ncol * nev

    def unpacked(buf, row):
        tops, bots = [], []
        for p in range(ncol // 2):
            a, b = buf[row * ncol + 2 * p], buf[row * ncol + 2 * p + 1]
            tops.append(jnp.where(low, a, half_roll(b)))
            bots.append(jnp.where(low, half_roll(a), b))
        value = jnp.concatenate([jnp.concatenate(tops, axis=1), jnp.concatenate(bots, axis=1)], axis=0)
        return jnp.concatenate(split(value), axis=0)

    def plus(total, part):
        return part if total is None else total + part

    def take_in(row, total):
        lanes = pl.ds(pl.multiple_of(row * depth, depth), depth)
        return plus(total, matmul(unpacked(gathered, row), hot_in[:, lanes], NT))

    def take_out(row, total):
        at = pl.ds(pl.multiple_of(row * depth, depth), depth)
        return plus(total, matmul(unpacked(solved, row), hot_out[at], NN))

    start1, relay1, finish1, drain1 = spread(gathered, ag1_send, ag1_recv, ag1_rest, near)
    pl.semaphore_wait(passed, nrow // 2 - 1)
    start1()

    loads[2].wait()
    local = jnp.concatenate([res_ref[...], inc], axis=1)
    out_ref[...] = matmul(local, linv[...], NT)
    relay1(1, ncol // 2)
    chunk = 2 * LANES
    loads[5].wait()

    def build_in(i):
        lanes = pl.ds(i * chunk if isinstance(i, int) else pl.multiple_of(i * chunk, chunk), chunk)
        slot = slots_ref[:, lanes] - c * width
        place = lax.broadcasted_iota(jnp.int32, (width, chunk), 0)
        hot_in[:, lanes] = jnp.where(place == slot, 1.0, 0.0).astype(BF16)

    loop(0, total // chunk, build_in)
    relay1(ncol // 2, ncol)
    loads[1].wait()
    a_hi, a_lo = split(coarse[...])
    coarse_hi[...] = a_hi
    coarse_lo[...] = a_lo
    column = finish1(take_in)
    for d in range(4):
        @pl.when(exists[opposite[d]])
        def _():
            lend(d).start()

    column_hi, column_lo = split(column[:rhs] + column[rhs:])
    column2 = jnp.concatenate([column_hi, column_lo], axis=0)
    span = 2 * LANES

    def product(i):
        at = pl.ds(i * span if isinstance(i, int) else pl.multiple_of(i * span, span), span)
        part = matmul(column2, coarse_hi[at], NT) + matmul(column2, coarse_lo[at], NT)
        part = part[:rhs] + part[rhs:]
        for q in range(span // LANES):
            top = part[:half, q * LANES:(q + 1) * LANES]
            bot = part[half:, q * LANES:(q + 1) * LANES]
            pieces[(span // LANES * i + q) * 2] = jnp.where(low, top, half_roll(bot))
            pieces[(span // LANES * i + q) * 2 + 1] = jnp.where(low, half_roll(top), bot)

    loop(0, rows // span, product)

    def reduce(k):
        peer = flipped(c, k, ncol)
        return pltpu.make_async_remote_copy(
            src_ref=pieces.at[peer], dst_ref=received.at[c],
            send_sem=rs_send.at[0], recv_sem=rs_recv.at[0],
            device_id=(r, peer), device_id_type=MESH)

    loop(1, ncol, lambda i: reduce(ncol - i).start())

    low8 = lane_low((8, LANES))

    def slots_of(device):
        device = jnp.clip(device, 0, ndev - 1)
        at = pl.ds(pl.multiple_of((device // 2) * LANES, LANES), LANES)
        pair = jnp.broadcast_to(slots_ref[:, at], (8, LANES))
        swapped = half_roll(pair)
        return jnp.where(lax.rem(device, 2) == 0, jnp.where(low8, pair, swapped), jnp.where(low8, swapped, pair))

    mine = [
        jnp.where(low8, slots_of(me), slots_of(me + ncol))[:1],
        jnp.where(low8, slots_of(me - ncol), slots_of(me + 1))[:1],
        jnp.where(low8, slots_of(me - 1), -1)[:1],
    ]
    tall = 4 * LANES

    def build_out(i):
        at = pl.ds(i * tall if isinstance(i, int) else pl.multiple_of(i * tall, tall), tall)
        place = lax.broadcasted_iota(jnp.int32, (tall, LANES), 0) + i * tall
        for q in range(3):
            hot_out[at, q * LANES:(q + 1) * LANES] = jnp.where(place == mine[q], 1.0, 0.0).astype(BF16)

    loop(0, total // tall, build_out)

    wide_hi[:nev] = basis2[:nev, :own]
    wide_lo[:nev] = basis2[nev:, :own]
    wide_hi[5 * nev:] = jnp.zeros_like(wide_hi[5 * nev:])
    wide_lo[5 * nev:] = jnp.zeros_like(wide_lo[5 * nev:])
    for d in range(4):
        @pl.when(exists[d])
        def _():
            lend(d).wait_recv()

        l_hi, l_lo = split(lent[d])
        for b in range(own // BLK):
            here = ib_ref[0, d] == b
            at = slice((d + 1) * nev, (d + 2) * nev), slice(b * BLK, (b + 1) * BLK)
            wide_hi[at] = jnp.where(here, l_hi, jnp.zeros_like(l_hi))
            wide_lo[at] = jnp.where(here, l_lo, jnp.zeros_like(l_lo))

    others = received.at[pl.ds(0, ncol - 1)]
    pltpu.make_async_copy(others, others, rs_recv.at[0]).wait()
    summed = pieces[c]
    if ncol - 1 <= UNROLL:
        for k in range(1, ncol):
            summed = summed + received[flipped(c, k, ncol)]
    else:
        summed = lax.fori_loop(1, ncol, lambda k, acc: acc + received[flipped(c, k, ncol)], summed)
    solved[me] = summed

    start2, relay2, finish2, drain2 = spread(solved, ag2_send, ag2_recv, ag2_rest, near)
    start2()
    relay2(1, ncol)
    picked = finish2(take_out)
    picked = picked.astype(BF16)

    inner = matmul(picked, wide_hi[...], NN) + matmul(picked, wide_lo[...], NN)
    out_ref[...] = out_ref[...] + inner[:rhs] + inner[rhs:]

    drain1()
    drain2()
    pltpu.make_async_copy(others, others, rs_send.at[0]).wait()
    for d in range(4):
        @pl.when(exists[d])
        def _():
            halo(d).wait_send()

        @pl.when(exists[opposite[d]])
        def _():
            lend(d).wait_send()


def shards(nrow, ncol, residuals, intersect_blocks, local_inverse, coarse_basis, coarse_slots, coarse_inverse):
    own, rhs = residuals.shape
    loc, nev = coarse_basis.shape
    rows, width = coarse_inverse.shape
    total = coarse_slots.shape[0]
    ndev = nrow * ncol
    assert 2 * nev == LANES and rows == ncol * nev and loc == own + 4 * BLK and own % BLK == 0
    packed = (rhs // 2, LANES)
    vmem = pl.BlockSpec(memory_space=pltpu.VMEM)
    hbm = pl.BlockSpec(memory_space=pl.ANY)
    dma = pltpu.SemaphoreType.DMA
    out = pl.pallas_call(
        functools.partial(kernel, nrow, ncol),
        name="schwarz",
        out_shape=pltpu.VMEM((rhs, own), F32),
        in_specs=[hbm] * 6,
        out_specs=vmem,
        scratch_shapes=[
            pltpu.VMEM((rhs, own), BF16),
            pltpu.SMEM(intersect_blocks.shape, jnp.int32),
            pltpu.VMEM((1, total), jnp.int32),
            pltpu.VMEM((4, rhs, BLK), BF16),
            pltpu.VMEM((4, rhs, BLK), BF16),
            pltpu.VMEM((own, loc), BF16),
            pltpu.VMEM((nev, loc), F32),
            pltpu.VMEM((2 * nev, loc), BF16),
            pltpu.VMEM((rows, width), F32),
            pltpu.VMEM((rows, width), BF16),
            pltpu.VMEM((rows, width), BF16),
            pltpu.VMEM((width, total), BF16),
            pltpu.VMEM((total, 3 * LANES), BF16),
            pltpu.VMEM((ndev,) + packed, F32),
            pltpu.VMEM((ncol,) + packed, F32),
            pltpu.VMEM((ncol,) + packed, F32),
            pltpu.VMEM((ndev,) + packed, F32),
            pltpu.VMEM((4, nev, BLK), F32),
            pltpu.VMEM((6 * nev, own), BF16),
            pltpu.VMEM((6 * nev, own), BF16),
            pltpu.SemaphoreType.REGULAR,
            dma((6,)),
            dma((4,)),
            dma((4,)),
            dma((4,)),
            dma((4,)),
            dma((1,)),
            dma((ncol, nrow // 2)),
            dma((nrow,)),
            dma((1,)),
            dma((1,)),
            dma((1,)),
            dma((ncol, nrow // 2)),
            dma((nrow,)),
        ],
        compiler_params=pltpu.CompilerParams(collective_id=0, has_side_effects=True),
    )(
        residuals.T,
        intersect_blocks,
        local_inverse,
        coarse_basis.T,
        coarse_slots.reshape(1, total),
        coarse_inverse,
    )
    return out.T


def solution(mesh):
    placed = (
        P(("row", "col"), None),
        P(("row", "col"), None),
        P(("row", "col"), None),
        P(("row", "col"), None),
        P(),
        P("row", "col"),
    )
    return jax.shard_map(
        functools.partial(shards, mesh.shape["row"], mesh.shape["col"]),
        mesh=mesh, in_specs=placed, out_specs=P(("row", "col"), None), check_vma=False,
    )
```

```python
import functools

import jax
import jax.numpy as jnp
from jax import lax
from jax.experimental import pallas as pl
from jax.experimental.pallas import tpu as pltpu
from jax.sharding import PartitionSpec as P

MESH = pl.DeviceIdType.MESH
BLK = 128
LANES = 128
UNROLL = 16
FAR_NUM, FAR_DEN = 1, 2
NT = (((1,), (1,)), ((), ()))
NN = (((1,), (0,)), ((), ()))
F32 = jnp.float32
BF16 = jnp.bfloat16


def matmul(a, b, dims):
    return lax.dot_general(a, b, dims, preferred_element_type=F32)


def split(x):
    hi = x.astype(BF16)
    return hi, (x - hi.astype(F32)).astype(BF16)


def loop(start, stop, body):
    if stop - start <= UNROLL:
        for i in range(start, stop):
            body(i)
    else:
        def step(i, carry):
            body(i)
            return carry

        lax.fori_loop(start, stop, step, 0)


def flipped(index, k, count):
    out = index
    bit = 1
    while bit < count:
        kbit = (k // bit) % 2
        out = out + kbit * bit * (1 - 2 * ((index // bit) % 2))
        bit *= 2
    return out


def lane_low(shape):
    return lax.broadcasted_iota(jnp.int32, shape, len(shape) - 1) < LANES // 2


def half_roll(x):
    return pltpu.roll(x, LANES // 2, 1)


def kernel(
    nrow,
    ncol,
    res_hbm,
    ib_hbm,
    linv_hbm,
    basis_hbm,
    slots_hbm,
    coarse_hbm,
    out_ref,
    res_ref,
    ib_ref,
    slots_ref,
    outgoing,
    incoming,
    linv,
    basis,
    basis2,
    coarse,
    coarse_hi,
    coarse_lo,
    hot_in,
    hot_out,
    gathered,
    pieces,
    received,
    solved,
    lent,
    wide_hi,
    wide_lo,
    passed,
    load_sem,
    halo_send,
    halo_recv,
    lend_send,
    lend_recv,
    ag1_send,
    ag1_recv,
    ag1_rest,
    rs_send,
    rs_recv,
    ag2_send,
    ag2_recv,
    ag2_rest,
):
    r = lax.axis_index("row")
    c = lax.axis_index("col")
    me = r * ncol + c
    rhs = res_ref.shape[0]
    own = res_ref.shape[1]
    half = rhs // 2
    ndev = nrow * ncol
    rows, width = coarse.shape
    total = slots_ref.shape[1]

    near = ncol * FAR_NUM // FAR_DEN

    def col_peer(k):
        return (r, flipped(c, k, ncol))

    def row_peer(j):
        return (lax.rem(r + j, nrow), c)

    barrier = pltpu.get_barrier_semaphore()
    loop(1, ncol, lambda k: pl.semaphore_signal(barrier, inc=1, device_id=col_peer(ncol - k), device_id_type=MESH))
    loop(1, nrow, lambda j: pl.semaphore_signal(barrier, inc=1, device_id=row_peer(j), device_id_type=MESH))

    loads = [
        pltpu.make_async_copy(basis_hbm, basis, load_sem.at[0]),
        pltpu.make_async_copy(coarse_hbm, coarse, load_sem.at[1]),
        pltpu.make_async_copy(linv_hbm, linv, load_sem.at[2]),
        pltpu.make_async_copy(res_hbm, res_ref, load_sem.at[3]),
        pltpu.make_async_copy(ib_hbm, ib_ref, load_sem.at[4]),
        pltpu.make_async_copy(slots_hbm, slots_ref, load_sem.at[5]),
    ]
    for load in loads[3:] + loads[:3]:
        load.start()
    loads[4].wait()
    loads[3].wait()

    exists = [r < nrow - 1, r > 0, c < ncol - 1, c > 0]
    target = [(r + 1, c), (r - 1, c), (r, c + 1), (r, c - 1)]
    opposite = [1, 0, 3, 2]
    blocks = [res_ref[:, b * BLK:(b + 1) * BLK] for b in range(own // BLK)]
    for d in range(4):
        index = ib_ref[0, d]
        value = blocks[0]
        for b in range(1, len(blocks)):
            value = jnp.where(index == b, blocks[b], value)
        outgoing[d] = value

        @pl.when(jnp.logical_not(exists[opposite[d]]))
        def _():
            incoming[d] = jnp.zeros_like(incoming[d])

        @pl.when(jnp.logical_not(exists[d]))
        def _():
            lent[d] = jnp.zeros_like(lent[d])

    def halo(d):
        return pltpu.make_async_remote_copy(
            src_ref=outgoing.at[d], dst_ref=incoming.at[d],
            send_sem=halo_send.at[d], recv_sem=halo_recv.at[d],
            device_id=target[d], device_id_type=MESH)

    def lend(d):
        return pltpu.make_async_remote_copy(
            src_ref=basis.at[:, pl.ds(own + d * BLK, BLK)], dst_ref=lent.at[d],
            send_sem=lend_send.at[d], recv_sem=lend_recv.at[d],
            device_id=target[opposite[d]], device_id_type=MESH)

    pl.semaphore_wait(barrier, ncol + nrow - 2)
    for q in range(1, nrow // 2):
        pl.semaphore_signal(passed, inc=1, device_id=(lax.rem(r + 2 * q, nrow), c), device_id_type=MESH)
    for d in range(4):
        @pl.when(exists[d])
        def _():
            halo(d).start()

    loads[0].wait()
    nev = basis.shape[0]
    b_hi, b_lo = split(basis[...])
    basis2[:nev] = b_hi
    basis2[nev:] = b_lo
    partial = matmul(res_ref[...], basis2[:, :own], NT)

    for d in range(4):
        @pl.when(exists[opposite[d]])
        def _():
            halo(d).wait_recv()

    inc = jnp.concatenate([incoming[d] for d in range(4)], axis=1)
    partial = partial + matmul(inc, basis2[:, own:], NT)
    partial = partial + half_roll(partial)
    low = lane_low((half, LANES))
    gathered[me] = jnp.where(low, partial[:half], partial[half:])

    def spread(buf, send, recv, rest, far):
        pairs = nrow // 2
        partner = r + 1 - 2 * lax.rem(r, 2)
        singles = ncol - 1 + (pairs - 1) * (ncol - far)

        def copy(slot, sem, device):
            return pltpu.make_async_remote_copy(
                src_ref=buf.at[slot], dst_ref=buf.at[slot], send_sem=send.at[0], recv_sem=sem,
                device_id=device, device_id_type=MESH)

        def pair_row(q):
            return lax.rem(r + 2 * q, nrow)

        def start():
            def one(i):
                k = ncol - i
                for q in range(pairs if i <= ncol - far else 1):
                    copy(me, recv.at[k, q], (pair_row(q), flipped(c, k, ncol))).start()

            if far == ncol:
                loop(1, ncol, lambda i: copy(me, recv.at[ncol - i, 0], col_peer(ncol - i)).start())
            else:
                for i in range(1, ncol):
                    one(i)
            share(r * ncol + c)

        def share(slot):
            for q in range(1, pairs):
                copy(slot, rest.at[pairs - q], (pair_row(q), c)).start()
            for q in range(1, pairs):
                copy(slot, rest.at[2 * pairs - q], (lax.rem(partner + 2 * q, nrow), c)).start()
            copy(slot, rest.at[pairs], (partner, c)).start()

        def arrival(slot, k, q):
            copy(slot, recv.at[k, q], (partner, c)).wait_recv()

        def relay(first, last):
            def near(k):
                slot = r * ncol + flipped(c, k, ncol)
                arrival(slot, k, 0)
                share(slot)

            def distant(k):
                for q in range(pairs):
                    slot = pair_row(pairs - q) * ncol + flipped(c, k, ncol)
                    arrival(slot, k, q)
                    copy(slot, rest.at[pairs + (pairs - q) % pairs], (partner, c)).start()

            loop(first, min(last, far), near)
            if last > far:
                loop(max(first, far), last, distant)

        def finish(consume):
            def wait(index, count):
                some = buf.at[pl.ds(0, count)]
                pltpu.make_async_copy(some, some, rest.at[index]).wait()

            total = consume(r, None)
            wait(pairs, ncol)
            total = consume(partner, total)
            for o in range(1, pairs):
                wait(o, far)
                total = consume(pair_row(o), total)
            for o in range(1, pairs):
                wait(pairs + o, ncol)
                total = consume(lax.rem(partner + 2 * o, nrow), total)
            return total

        def drain():
            count = singles + far * (nrow - 1) + (ncol - far) * pairs
            while count > 0:
                now = min(count, ndev)
                some = buf.at[pl.ds(0, now)]
                pltpu.make_async_copy(some, some, send.at[0]).wait()
                count -= now

        return start, relay, finish, drain

    depth = ncol * nev

    def unpacked(buf, row):
        tops, bots = [], []
        for p in range(ncol // 2):
            a, b = buf[row * ncol + 2 * p], buf[row * ncol + 2 * p + 1]
            tops.append(jnp.where(low, a, half_roll(b)))
            bots.append(jnp.where(low, half_roll(a), b))
        value = jnp.concatenate([jnp.concatenate(tops, axis=1), jnp.concatenate(bots, axis=1)], axis=0)
        return jnp.concatenate(split(value), axis=0)

    def plus(total, part):
        return part if total is None else total + part

    def take_in(row, total):
        lanes = pl.ds(pl.multiple_of(row * depth, depth), depth)
        return plus(total, matmul(unpacked(gathered, row), hot_in[:, lanes], NT))

    def take_out(row, total):
        at = pl.ds(pl.multiple_of(row * depth, depth), depth)
        return plus(total, matmul(unpacked(solved, row), hot_out[at], NN))

    start1, relay1, finish1, drain1 = spread(gathered, ag1_send, ag1_recv, ag1_rest, near)
    pl.semaphore_wait(passed, nrow // 2 - 1)
    start1()

    loads[2].wait()
    local = jnp.concatenate([res_ref[...], inc], axis=1)
    out_ref[...] = matmul(local, linv[...], NT)
    relay1(1, ncol // 2)
    chunk = 2 * LANES
    loads[5].wait()

    def build_in(i):
        lanes = pl.ds(i * chunk if isinstance(i, int) else pl.multiple_of(i * chunk, chunk), chunk)
        slot = slots_ref[:, lanes] - c * width
        place = lax.broadcasted_iota(jnp.int32, (width, chunk), 0)
        hot_in[:, lanes] = jnp.where(place == slot, 1.0, 0.0).astype(BF16)

    loop(0, total // chunk, build_in)
    relay1(ncol // 2, ncol)
    loads[1].wait()
    a_hi, a_lo = split(coarse[...])
    coarse_hi[...] = a_hi
    coarse_lo[...] = a_lo
    column = finish1(take_in)
    for d in range(4):
        @pl.when(exists[opposite[d]])
        def _():
            lend(d).start()

    column_hi, column_lo = split(column[:rhs] + column[rhs:])
    column2 = jnp.concatenate([column_hi, column_lo], axis=0)
    span = 2 * LANES

    def reduce(peer):
        return pltpu.make_async_remote_copy(
            src_ref=pieces.at[peer], dst_ref=received.at[c],
            send_sem=rs_send.at[0], recv_sem=rs_recv.at[0],
            device_id=(r, peer), device_id_type=MESH)

    group = 2 * (span // LANES)

    def product(i):
        block = lax.rem(c // group + 1 + i, rows // span)
        at = pl.ds(pl.multiple_of(block * span, span), span)
        part = matmul(column2, coarse_hi[at], NT) + matmul(column2, coarse_lo[at], NT)
        part = part[:rhs] + part[rhs:]
        for q in range(span // LANES):
            top = part[:half, q * LANES:(q + 1) * LANES]
            bot = part[half:, q * LANES:(q + 1) * LANES]
            pieces[block * group + 2 * q] = jnp.where(low, top, half_roll(bot))
            pieces[block * group + 2 * q + 1] = jnp.where(low, half_roll(top), bot)

        for q in range(group):
            @pl.when(block * group + q != c)
            def _():
                reduce(block * group + q).start()

    loop(0, rows // span, product)

    low8 = lane_low((8, LANES))

    def slots_of(device):
        device = jnp.clip(device, 0, ndev - 1)
        at = pl.ds(pl.multiple_of((device // 2) * LANES, LANES), LANES)
        pair = jnp.broadcast_to(slots_ref[:, at], (8, LANES))
        swapped = half_roll(pair)
        return jnp.where(lax.rem(device, 2) == 0, jnp.where(low8, pair, swapped), jnp.where(low8, swapped, pair))

    mine = [
        jnp.where(low8, slots_of(me), slots_of(me + ncol))[:1],
        jnp.where(low8, slots_of(me - ncol), slots_of(me + 1))[:1],
        jnp.where(low8, slots_of(me - 1), -1)[:1],
    ]
    tall = 4 * LANES

    def build_out(i):
        at = pl.ds(i * tall if isinstance(i, int) else pl.multiple_of(i * tall, tall), tall)
        place = lax.broadcasted_iota(jnp.int32, (tall, LANES), 0) + i * tall
        for q in range(3):
            hot_out[at, q * LANES:(q + 1) * LANES] = jnp.where(place == mine[q], 1.0, 0.0).astype(BF16)

    loop(0, total // tall, build_out)

    wide_hi[:nev] = basis2[:nev, :own]
    wide_lo[:nev] = basis2[nev:, :own]
    wide_hi[5 * nev:] = jnp.zeros_like(wide_hi[5 * nev:])
    wide_lo[5 * nev:] = jnp.zeros_like(wide_lo[5 * nev:])
    for d in range(4):
        @pl.when(exists[d])
        def _():
            lend(d).wait_recv()

        l_hi, l_lo = split(lent[d])
        for b in range(own // BLK):
            here = ib_ref[0, d] == b
            at = slice((d + 1) * nev, (d + 2) * nev), slice(b * BLK, (b + 1) * BLK)
            wide_hi[at] = jnp.where(here, l_hi, jnp.zeros_like(l_hi))
            wide_lo[at] = jnp.where(here, l_lo, jnp.zeros_like(l_lo))

    others = received.at[pl.ds(0, ncol - 1)]
    pltpu.make_async_copy(others, others, rs_recv.at[0]).wait()
    summed = pieces[c]
    if ncol - 1 <= UNROLL:
        for k in range(1, ncol):
            summed = summed + received[flipped(c, k, ncol)]
    else:
        summed = lax.fori_loop(1, ncol, lambda k, acc: acc + received[flipped(c, k, ncol)], summed)
    solved[me] = summed

    start2, relay2, finish2, drain2 = spread(solved, ag2_send, ag2_recv, ag2_rest, near)
    start2()
    relay2(1, ncol)
    picked = finish2(take_out)
    picked = picked.astype(BF16)

    inner = matmul(picked, wide_hi[...], NN) + matmul(picked, wide_lo[...], NN)
    out_ref[...] = out_ref[...] + inner[:rhs] + inner[rhs:]

    drain1()
    drain2()
    pltpu.make_async_copy(others, others, rs_send.at[0]).wait()
    for d in range(4):
        @pl.when(exists[d])
        def _():
            halo(d).wait_send()

        @pl.when(exists[opposite[d]])
        def _():
            lend(d).wait_send()


def shards(nrow, ncol, residuals, intersect_blocks, local_inverse, coarse_basis, coarse_slots, coarse_inverse):
    own, rhs = residuals.shape
    loc, nev = coarse_basis.shape
    rows, width = coarse_inverse.shape
    total = coarse_slots.shape[0]
    ndev = nrow * ncol
    assert 2 * nev == LANES and rows == ncol * nev and loc == own + 4 * BLK and own % BLK == 0
    packed = (rhs // 2, LANES)
    vmem = pl.BlockSpec(memory_space=pltpu.VMEM)
    hbm = pl.BlockSpec(memory_space=pl.ANY)
    dma = pltpu.SemaphoreType.DMA
    out = pl.pallas_call(
        functools.partial(kernel, nrow, ncol),
        name="schwarz",
        out_shape=pltpu.VMEM((rhs, own), F32),
        in_specs=[hbm] * 6,
        out_specs=vmem,
        scratch_shapes=[
            pltpu.VMEM((rhs, own), BF16),
            pltpu.SMEM(intersect_blocks.shape, jnp.int32),
            pltpu.VMEM((1, total), jnp.int32),
            pltpu.VMEM((4, rhs, BLK), BF16),
            pltpu.VMEM((4, rhs, BLK), BF16),
            pltpu.VMEM((own, loc), BF16),
            pltpu.VMEM((nev, loc), F32),
            pltpu.VMEM((2 * nev, loc), BF16),
            pltpu.VMEM((rows, width), F32),
            pltpu.VMEM((rows, width), BF16),
            pltpu.VMEM((rows, width), BF16),
            pltpu.VMEM((width, total), BF16),
            pltpu.VMEM((total, 3 * LANES), BF16),
            pltpu.VMEM((ndev,) + packed, F32),
            pltpu.VMEM((ncol,) + packed, F32),
            pltpu.VMEM((ncol,) + packed, F32),
            pltpu.VMEM((ndev,) + packed, F32),
            pltpu.VMEM((4, nev, BLK), F32),
            pltpu.VMEM((6 * nev, own), BF16),
            pltpu.VMEM((6 * nev, own), BF16),
            pltpu.SemaphoreType.REGULAR,
            dma((6,)),
            dma((4,)),
            dma((4,)),
            dma((4,)),
            dma((4,)),
            dma((1,)),
            dma((ncol, nrow // 2)),
            dma((nrow,)),
            dma((1,)),
            dma((1,)),
            dma((1,)),
            dma((ncol, nrow // 2)),
            dma((nrow,)),
        ],
        compiler_params=pltpu.CompilerParams(collective_id=0, has_side_effects=True),
    )(
        residuals.T,
        intersect_blocks,
        local_inverse,
        coarse_basis.T,
        coarse_slots.reshape(1, total),
        coarse_inverse,
    )
    return out.T


def solution(mesh):
    placed = (
        P(("row", "col"), None),
        P(("row", "col"), None),
        P(("row", "col"), None),
        P(("row", "col"), None),
        P(),
        P("row", "col"),
    )
    return jax.shard_map(
        functools.partial(shards, mesh.shape["row"], mesh.shape["col"]),
        mesh=mesh, in_specs=placed, out_specs=P(("row", "col"), None), check_vma=False,
    )
```
